32 devices in a mesh: dp: 8 (over y, x, core), tp: 4 (over z).
Axes of the slice: x: 2, y: 2, z: 4, core: 2. Of those that a mesh axis runs over, the one named last changes fastest.
Arguments:
- resid: bfloat16 [2048, 4096], P('dp'), may hold values from -6 to 6
- gain: bfloat16 [4096], replicated, may hold values from 0.25 to 1.75
- grad_q: bfloat16 [2048, 3072], P('dp', 'tp'), may hold values from -1.25 to 1.25
- w_query: bfloat16 [3072, 4096], P('tp'), may hold values from -0.375 to 0.375
- grad_in: bfloat16 [2048, 4096], P('dp'), may hold values from -2 to 2
Outputs:
- weight_grad: float32 [3072, 4096], P(('tp', 'dp'))
- gain_grad: float32 [4096], replicated
- grad_out: bfloat16 [2048, 4096], P('dp')
The draws below stay inside these ranges and needn't reach their ends.
All inputs are finite; a program needn't handle non-finite values.
Results may differ from the reference program's by a relative error of at most 0.014.
Values may be sent and summed in bfloat16 or wider, within the bound.
A program may use at most 128 MiB of HBM per device.

```python
import jax
import jax.numpy as jnp
from jax import lax

D = 4096
QW = 3072
TOKENS = 2048
N_TP = 4


def with_spikes(drawn, stream_key, source, target, parts, factor):
    owner, partner = [(jnp.arange(drawn.shape[dim]) // (drawn.shape[dim] // parts)).reshape([-1 if axis == dim else 1 for axis in range(drawn.ndim)]) for dim in (source, target)]
    chosen = jax.random.permutation(stream_key, parts)[partner]
    strong = (owner == chosen) | (owner == (partner + parts // 2) % parts)
    return jnp.where(strong, factor * drawn, drawn)


def shard_levels(key, dims, cuts, low, top_value):
    def one(dim, parts):
        draws = jax.random.uniform(jax.random.fold_in(jax.random.fold_in(key, 6), dim), (parts,), jnp.float32, low / len(cuts), top_value / len(cuts))
        return jnp.repeat(jnp.exp(draws), dims[dim] // parts).reshape((-1,) + (1,) * (len(dims) - dim - 1))

    level = one(*cuts[0])
    for cut in cuts[1:]:
        level = level * one(*cut)
    return level


def gaussian(own_key, extent, scale, bound, split=(), dtype=jnp.bfloat16):
    drawn = scale * jax.random.normal(own_key, extent, jnp.float32)
    if split:
        drawn = drawn * shard_levels(own_key, extent, split, -0.22, 0.18)
    return jnp.clip(drawn, -bound, bound).astype(dtype)


def gaussian_with(stream_key, dims, deviation, reach, split, heavy, kind=jnp.bfloat16):
    values = deviation * jax.random.normal(stream_key, dims, jnp.float32)
    if split:
        values = values * shard_levels(stream_key, dims, split, -0.22, 0.18)
    return jnp.clip(with_spikes(values, jax.random.fold_in(stream_key, 3), *heavy), -reach, reach).astype(kind)


def setup_inputs(seed: int = 0) -> dict:
    streams_of = jax.random.split(jax.random.key(seed), 6)
    resid = gaussian(streams_of[0], (TOKENS, D), 1.0, 6.0, ((0, 8),))
    gain = jnp.clip(1.0 + 0.15 * jax.random.normal(streams_of[1], (D,), jnp.float32), 0.25, 1.75).astype(jnp.bfloat16)
    grad_q = gaussian_with(streams_of[2], (TOKENS, QW), 0.0625, 1.25, ((0, 8), (1, 4)), (0, 1, 8, 2.0))
    w_query = gaussian(streams_of[3], (QW, D), (D // 16) ** -0.5, 0.375, ((0, 4),))
    grad_in = gaussian(streams_of[4], (TOKENS, D), 0.125, 2.0, ((0, 8),))
    return dict(resid=resid, gain=gain, grad_q=grad_q, w_query=w_query, grad_in=grad_in)


def reference(resid, gain, grad_q, w_query, grad_in):
    resid_f = resid.astype(jnp.float32)
    gain_f = gain.astype(jnp.float32)
    inv_rms = lax.rsqrt(lax.optimization_barrier(jnp.mean(resid_f * resid_f, axis=-1, keepdims=True)) + 1e-05)
    unit = resid_f * inv_rms
    normed = (unit * gain_f).astype(jnp.bfloat16)
    weight_grad = jnp.dot(grad_q.astype(jnp.float32).T, normed.astype(jnp.float32), preferred_element_type=jnp.float32)
    block = QW // N_TP
    dnormed = jnp.zeros(resid.shape, jnp.float32)
    for index in range(N_TP):
        cols = grad_q[:, index * block:(index + 1) * block].astype(jnp.float32)
        rows = w_query[index * block:(index + 1) * block, :].astype(jnp.float32)
        partial_value = jnp.dot(cols, rows, preferred_element_type=jnp.float32).astype(jnp.bfloat16)
        dnormed = dnormed + partial_value.astype(jnp.float32)
    gain_grad = lax.optimization_barrier(jnp.sum(dnormed * unit, axis=0))
    dunit = dnormed * gain_f
    inner = lax.optimization_barrier(jnp.mean(dunit * unit, axis=-1, keepdims=True))
    grad_out = (grad_in.astype(jnp.float32) + inv_rms * (dunit - unit * inner)).astype(jnp.bfloat16)
    return (weight_grad, gain_grad, grad_out)
```

```python
import functools

import jax
import jax.numpy as jnp
from jax import lax
from jax.experimental import pallas as pl
from jax.experimental.pallas import tpu as pltpu
from jax.sharding import PartitionSpec as P

MESH = pl.DeviceIdType.MESH
F32 = jnp.float32
BF16 = jnp.bfloat16
ROWS = 16
TILES = 8


def norm_rows(rows_bf, gain_f):
    rows_f = rows_bf.astype(jnp.float32)
    inv_rms = lax.rsqrt(jnp.mean(rows_f * rows_f, axis=-1, keepdims=True) + 1e-05)
    unit = rows_f * inv_rms
    return (inv_rms, unit, (unit * gain_f).astype(jnp.bfloat16))


def per_device(resid, gain, grad_q, w_query, grad_in):
    gain_f = gain.astype(jnp.float32)
    inv_rms, unit, normed = norm_rows(resid, gain_f)
    local_term = jnp.dot(grad_q, w_query, preferred_element_type=jnp.float32)
    dnormed = lax.psum(local_term.astype(jnp.bfloat16), "tp").astype(jnp.float32)
    full_grad = lax.dot_general(
        grad_q, normed, (((0,), (0,)), ((), ())), preferred_element_type=jnp.float32
    )
    weight_grad = lax.psum_scatter(full_grad, "dp", scatter_dimension=0, tiled=True)
    gain_grad = lax.psum(jnp.sum(dnormed * unit, axis=0), "dp")
    dunit = dnormed * gain_f
    inner = jnp.mean(dunit * unit, axis=-1, keepdims=True)
    grad_rows = (grad_in.astype(jnp.float32) + inv_rms * (dunit - unit * inner)).astype(
        jnp.bfloat16
    )
    return (weight_grad, gain_grad, grad_rows)


def kernel(n_dp, n_tp, resid, gain, grad_q, w_query, grad_in, wg_out, gg_out, go_out,
           wv, rv, gqv, giv, nv, part, from_mate, from_peer, gq_t, gq_p,
           fgs, fgr, keep, xs, xr, ys, yr, wgo, gacc, gslot, gz,
           w_sem, in_sem, so, ro, sp, rp, out_sem, s1, r1, s2, r2, s3, r3, wg_sem, sg, rg, sz, rz):
    dp, tp = lax.axis_index("dp"), lax.axis_index("tp")
    tokens, width = rv.shape
    heads = gqv.shape[1]
    chunks = tokens // ROWS
    steps = chunks // 2
    cols = width // TILES
    block = heads // n_dp
    h = tp // 2
    is_inner = jnp.logical_and(tp > 0, tp < n_tp - 1)
    is_outer = jnp.logical_not(is_inner)
    mate = jnp.where(is_inner, h * (n_tp - 1), 1 + h)
    peer = 2 - h
    core, xx, yy = dp % 2, (dp // 2) % 2, dp // 4
    core_mate = dp + 1 - 2 * core
    x_mate = dp + 2 - 4 * xx
    y_mate = dp + 4 - 8 * yy

    def w_copy(t):
        c = pl.ds(t * cols, cols)
        return pltpu.make_async_copy(w_query.at[:, c], wv.at[:, c], w_sem.at[t])

    gq_copy = pltpu.make_async_copy(grad_q, gqv, in_sem.at[0])
    r_copy = pltpu.make_async_copy(resid, rv, in_sem.at[1])
    gi_copy = pltpu.make_async_copy(grad_in, giv, in_sem.at[2])
    gq_copy.start()
    for t in range(TILES):
        w_copy(t).start()
    r_copy.start()
    gi_copy.start()

    barrier = pltpu.get_barrier_semaphore()
    for o in range(1, n_dp):
        pl.semaphore_signal(barrier, inc=1, device_id={"dp": (dp + o) % n_dp}, device_id_type=MESH)
    for o in range(1, n_tp):
        pl.semaphore_signal(barrier, inc=1, device_id={"tp": (tp + o) % n_tp}, device_id_type=MESH)

    def rows_of(c):
        return pl.ds(pl.multiple_of(c * ROWS, ROWS), ROWS)

    def copy_o(src, c):
        return pltpu.make_async_remote_copy(
            src_ref=src.at[rows_of(c)], dst_ref=from_mate.at[rows_of(c)],
            send_sem=so.at[c], recv_sem=ro.at[c], device_id={"tp": mate}, device_id_type=MESH)

    def copy_p(src, c):
        return pltpu.make_async_remote_copy(
            src_ref=src.at[rows_of(c)], dst_ref=from_peer.at[rows_of(c)],
            send_sem=sp.at[c], recv_sem=rp.at[c], device_id={"tp": peer}, device_id_type=MESH)

    def out_copy(src, c):
        return pltpu.make_async_copy(src.at[rows_of(c)], go_out.at[rows_of(c)], out_sem.at[c])

    def hop(src, dst, send, recv, t, to):
        return pltpu.make_async_remote_copy(
            src_ref=src.at[t], dst_ref=dst.at[t], send_sem=send.at[t], recv_sem=recv.at[t],
            device_id={"dp": to}, device_id_type=MESH)

    gq_copy.wait()
    half = tokens // 2
    for m in range(2):
        for t in range(TILES):
            if m == 0:
                w_copy(t).wait()
            c = slice(t * cols, (t + 1) * cols)
            r = slice(m * half, (m + 1) * half)
            part[r, c] = jnp.dot(gqv[r, :], wv[:, c], preferred_element_type=F32).astype(BF16)
        if m == 0:
            pl.semaphore_wait(barrier, n_dp - 1 + n_tp - 1)

        @pl.when(is_outer)
        def _():
            @pl.loop(m * steps // 2, (m + 1) * steps // 2)
            def _(k):
                copy_o(part, 2 * k + 1 - h).start()
                copy_o(part, 2 * k + h).start()

    gain_f = gain[...].astype(F32)
    r_copy.wait()

    @pl.loop(0, chunks)
    def _(c):
        r = rows_of(c)
        nv[r, :] = norm_rows(rv[r, :], gain_f)[2]

    gq_t[...] = gqv[...].T
    for v in range(2):
        for j, rel in enumerate(((0, 2, 1, 3), (0, 1, 2, 3))[v]):
            y_to = yy + (rel // 2) * (1 - 2 * yy)
            x_to = xx + (rel % 2) * (1 - 2 * xx)
            for mine in range(2):
                c_to = core if mine else 1 - core
                at = pl.multiple_of((y_to * 4 + x_to * 2 + c_to) * block, block)
                gq_p[v, mine, j * block:(j + 1) * block, :] = gq_t[pl.ds(at, block), :]
    gacc[...] = jnp.zeros_like(gacc)
    first, second = (x_mate, y_mate), (y_mate, x_mate)

    def tile_cols(t):
        return pl.ds(pl.multiple_of(t * cols, cols), cols)

    @pl.loop(0, TILES // 2)
    def _(j):
        for v in range(2):
            t = 2 * j + v
            fgs[t] = jnp.dot(gq_p[v, 0], nv[:, tile_cols(t)], preferred_element_type=F32).astype(BF16)
            hop(fgs, fgr, s1, r1, t, core_mate).start()

    def stage2(j):
        for v in range(2):
            t = 2 * j + v
            hop(fgs, fgr, s1, r1, t, core_mate).wait_recv()
            total = jnp.dot(gq_p[v, 1], nv[:, tile_cols(t)], preferred_element_type=F32)
            total = total + fgr[t].astype(F32)
            xs[t] = total[2 * block:].astype(BF16)
            hop(xs, xr, s2, r2, t, first[v]).start()
            keep[t] = total[:2 * block]

    def stage3(j):
        for v in range(2):
            t = 2 * j + v
            hop(xs, xr, s2, r2, t, first[v]).wait_recv()
            ys[t] = (keep[t, block:] + xr[t, block:].astype(F32)).astype(BF16)
            hop(ys, yr, s3, r3, t, second[v]).start()
            keep[t, :block] = keep[t, :block] + xr[t, :block].astype(F32)

    def wg_copy(t):
        return pltpu.make_async_copy(wgo.at[t], wg_out.at[:, tile_cols(t)], wg_sem.at[t])

    def stage4(j):
        for v in range(2):
            t = 2 * j + v
            hop(ys, yr, s3, r3, t, second[v]).wait_recv()
            wgo[t] = keep[t, :block] + yr[t].astype(F32)
            wg_copy(t).start()

    gi_copy.wait()

    def forward(k):
        b = 2 * k + 1 - h
        copy_p(from_peer, b).wait_recv()
        copy_o(from_peer, b).start()
        out_copy(from_peer, b).start()

    def collect(k):
        for c in (2 * k + h, 2 * k + 1 - h):
            copy_o(from_mate, c).wait_recv()
            out_copy(from_mate, c).start()

    @pl.loop(0, steps)
    def _(k):
        @pl.when(is_inner)
        def _():
            a, b = 2 * k + h, 2 * k + 1 - h
            copy_o(part, b).wait_recv()
            part[rows_of(b), :] = (
                part[rows_of(b), :].astype(F32) + from_mate[rows_of(b), :].astype(F32)
            ).astype(BF16)
            copy_p(part, b).start()
            copy_o(part, a).wait_recv()
            copy_p(part, a).wait_recv()
            r = rows_of(a)
            inv_rms, unit, _ = norm_rows(rv[r, :], gain_f)
            dnormed = part[r, :].astype(F32) + from_mate[r, :].astype(F32)
            dnormed = dnormed + from_peer[r, :].astype(F32)
            gacc[...] += jnp.sum(dnormed * unit, axis=0, keepdims=True)
            dunit = dnormed * gain_f
            mean = jnp.mean(dunit * unit, axis=-1, keepdims=True)
            part[r, :] = (
                giv[r, :].astype(F32) + inv_rms * (dunit - unit * mean)
            ).astype(BF16)
            copy_p(part, a).start()
            copy_o(part, a).start()
            out_copy(part, a).start()

            @pl.when(k > 0)
            def _():
                forward(k - 1)

        @pl.when(jnp.logical_and(is_outer, k > 2))
        def _():
            collect(k - 3)

        @pl.when(k < 2)
        def _():
            stage2(2 * k)
            stage2(2 * k + 1)

        @pl.when(jnp.logical_and(k >= 2, k < 2 + TILES // 2))
        def _():
            stage3(k - 2)

        @pl.when(jnp.logical_and(k >= 4, k < 4 + TILES // 2))
        def _():
            stage4(k - 4)

    def g_copy(o):
        return pltpu.make_async_remote_copy(
            src_ref=gslot.at[0], dst_ref=gslot.at[o], send_sem=sg.at[o], recv_sem=rg.at[o],
            device_id={"dp": (dp + o) % n_dp}, device_id_type=MESH)

    def z_copy(i, to):
        return pltpu.make_async_remote_copy(
            src_ref=gz.at[h], dst_ref=gz.at[h], send_sem=sz.at[i], recv_sem=rz.at[h],
            device_id={"tp": to}, device_id_type=MESH)

    def z_wait(which):
        pltpu.make_async_remote_copy(
            src_ref=gz.at[which], dst_ref=gz.at[which], send_sem=sz.at[0], recv_sem=rz.at[which],
            device_id={"tp": mate}, device_id_type=MESH).wait_recv()

    @pl.when(is_inner)
    def _():
        gslot[0] = gacc[...]
        for o in range(1, n_dp):
            g_copy(o).start()
        forward(steps - 1)
        for o in range(1, n_dp):
            g_copy(o).wait_recv()
        total = gslot[dp % n_dp]
        for d in range(1, n_dp):
            total = total + gslot[(dp + n_dp - d) % n_dp]
        gz[h] = total
        targets = (mate, peer, (1 - h) * (n_tp - 1))
        for i, to in enumerate(targets):
            z_copy(i, to).start()
        z_wait(1 - h)
        gg_out[...] = gz[0] + gz[1]
        for i, to in enumerate(targets):
            z_copy(i, to).wait_send()
        for o in range(1, n_dp):
            g_copy(o).wait_send()

        @pl.loop(0, chunks)
        def _(c):
            copy_p(part, c).wait_send()

    @pl.when(is_outer)
    def _():
        for k in range(steps - 3, steps):
            collect(k)
        z_wait(0)
        z_wait(1)
        gg_out[...] = gz[0] + gz[1]

    @pl.loop(0, chunks)
    def _(c):
        copy_o(part, c).wait_send()
        out_copy(part, c).wait()

    for t in range(TILES):
        hop(fgs, fgr, s1, r1, t, core_mate).wait_send()
        hop(xs, xr, s2, r2, t, first[t % 2]).wait_send()
        hop(ys, yr, s3, r3, t, second[t % 2]).wait_send()
        wg_copy(t).wait()


def fused(n_dp, n_tp, resid, gain, grad_q, w_query, grad_in):
    tokens, width = resid.shape
    heads = grad_q.shape[1]
    chunks = tokens // ROWS
    block, cols = heads // n_dp, width // TILES
    any_space = pl.BlockSpec(memory_space=pl.ANY)
    vmem = pl.BlockSpec(memory_space=pltpu.VMEM)
    dma = lambda n: pltpu.SemaphoreType.DMA((n,))
    weight_grad, gain_grad, grad_rows = pl.pallas_call(
        functools.partial(kernel, n_dp, n_tp),
        out_shape=(
            jax.ShapeDtypeStruct((block, width), F32),
            jax.ShapeDtypeStruct((1, width), F32),
            jax.ShapeDtypeStruct((tokens, width), BF16),
        ),
        in_specs=[any_space, vmem, any_space, any_space, any_space],
        out_specs=(any_space, vmem, any_space),
        scratch_shapes=[
            pltpu.VMEM((heads, width), BF16),
            pltpu.VMEM((tokens, width), BF16),
            pltpu.VMEM((tokens, heads), BF16),
            pltpu.VMEM((tokens, width), BF16),
            pltpu.VMEM((tokens, width), BF16),
            pltpu.VMEM((tokens, width), BF16),
            pltpu.VMEM((tokens, width), BF16),
            pltpu.VMEM((tokens, width), BF16),
            pltpu.VMEM((heads, tokens), BF16),
            pltpu.VMEM((2, 2, 4 * block, tokens), BF16),
            pltpu.VMEM((TILES, 4 * block, cols), BF16),
            pltpu.VMEM((TILES, 4 * block, cols), BF16),
            pltpu.VMEM((TILES, 2 * block, cols), F32),
            pltpu.VMEM((TILES, 2 * block, cols), BF16),
            pltpu.VMEM((TILES, 2 * block, cols), BF16),
            pltpu.VMEM((TILES, block, cols), BF16),
            pltpu.VMEM((TILES, block, cols), BF16),
            pltpu.VMEM((TILES, block, cols), F32),
            pltpu.VMEM((1, width), F32),
            pltpu.VMEM((n_dp, 1, width), F32),
            pltpu.VMEM((2, 1, width), F32),
            dma(TILES), dma(3), dma(chunks), dma(chunks), dma(chunks), dma(chunks), dma(chunks),
            dma(TILES), dma(TILES), dma(TILES), dma(TILES), dma(TILES), dma(TILES), dma(TILES),
            dma(n_dp), dma(n_dp), dma(3), dma(2),
        ],
        compiler_params=pltpu.CompilerParams(
            collective_id=0, has_side_effects=True, vmem_limit_bytes=60 * 1024 * 1024
        ),
    )(resid, gain.reshape(1, width), grad_q, w_query, grad_in)
    return weight_grad, gain_grad.reshape(width), grad_rows


def solution(mesh):
    n_dp, n_tp = mesh.shape["dp"], mesh.shape["tp"]
    if (n_dp, n_tp) == (2 * 2 * 2, 4):
        body = functools.partial(fused, n_dp, n_tp)
    else:
        body = per_device
    return jax.shard_map(
        body,
        mesh=mesh,
        in_specs=(P("dp", None), P(), P("dp", "tp"), P("tp", None), P("dp", None)),
        out_specs=(P(("tp", "dp"), None), P(), P("dp", None)),
        check_vma=False,
    )
```

```python
import functools

import jax
import jax.numpy as jnp
from jax import lax
from jax.experimental import pallas as pl
from jax.experimental.pallas import tpu as pltpu
from jax.sharding import PartitionSpec as P

MESH = pl.DeviceIdType.MESH
F32 = jnp.float32
BF16 = jnp.bfloat16
ROWS = 16
TILES = 8


def norm_rows(rows_bf, gain_f):
    rows_f = rows_bf.astype(jnp.float32)
    inv_rms = lax.rsqrt(jnp.mean(rows_f * rows_f, axis=-1, keepdims=True) + 1e-05)
    unit = rows_f * inv_rms
    return (inv_rms, unit, (unit * gain_f).astype(jnp.bfloat16))


def per_device(resid, gain, grad_q, w_query, grad_in):
    gain_f = gain.astype(jnp.float32)
    inv_rms, unit, normed = norm_rows(resid, gain_f)
    local_term = jnp.dot(grad_q, w_query, preferred_element_type=jnp.float32)
    dnormed = lax.psum(local_term.astype(jnp.bfloat16), "tp").astype(jnp.float32)
    full_grad = lax.dot_general(
        grad_q, normed, (((0,), (0,)), ((), ())), preferred_element_type=jnp.float32
    )
    weight_grad = lax.psum_scatter(full_grad, "dp", scatter_dimension=0, tiled=True)
    gain_grad = lax.psum(jnp.sum(dnormed * unit, axis=0), "dp")
    dunit = dnormed * gain_f
    inner = jnp.mean(dunit * unit, axis=-1, keepdims=True)
    grad_rows = (grad_in.astype(jnp.float32) + inv_rms * (dunit - unit * inner)).astype(
        jnp.bfloat16
    )
    return (weight_grad, gain_grad, grad_rows)


def kernel(n_dp, n_tp, resid, gain, grad_q, w_query, grad_in, wg_out, gg_out, go_out,
           wv, rv, gqv, giv, nv, part, from_mate, from_peer, gq_t, gq_p,
           fgs, fgr, keep, xs, xr, ys, yr, wgo, gacc, gslot, gz,
           w_sem, in_sem, so, ro, sp, rp, out_sem, s1, r1, s2, r2, s3, r3, wg_sem, sg, rg, sz, rz):
    dp, tp = lax.axis_index("dp"), lax.axis_index("tp")
    tokens, width = rv.shape
    heads = gqv.shape[1]
    chunks = tokens // ROWS
    steps = chunks // 2
    cols = width // TILES
    block = heads // n_dp
    h = tp // 2
    is_inner = jnp.logical_and(tp > 0, tp < n_tp - 1)
    is_outer = jnp.logical_not(is_inner)
    mate = jnp.where(is_inner, h * (n_tp - 1), 1 + h)
    peer = 2 - h
    core, xx, yy = dp % 2, (dp // 2) % 2, dp // 4
    core_mate = dp + 1 - 2 * core
    x_mate = dp + 2 - 4 * xx
    y_mate = dp + 4 - 8 * yy

    def w_copy(t):
        c = pl.ds(t * cols, cols)
        return pltpu.make_async_copy(w_query.at[:, c], wv.at[:, c], w_sem.at[t])

    gq_copy = pltpu.make_async_copy(grad_q, gqv, in_sem.at[0])
    r_copy = pltpu.make_async_copy(resid, rv, in_sem.at[1])
    gi_copy = pltpu.make_async_copy(grad_in, giv, in_sem.at[2])
    gq_copy.start()
    for t in range(TILES):
        w_copy(t).start()
    r_copy.start()
    gi_copy.start()

    barrier = pltpu.get_barrier_semaphore()
    for o in range(1, n_dp):
        pl.semaphore_signal(barrier, inc=1, device_id={"dp": (dp + o) % n_dp}, device_id_type=MESH)
    for o in range(1, n_tp):
        pl.semaphore_signal(barrier, inc=1, device_id={"tp": (tp + o) % n_tp}, device_id_type=MESH)

    def rows_of(c):
        return pl.ds(pl.multiple_of(c * ROWS, ROWS), ROWS)

    def copy_o(src, c):
        return pltpu.make_async_remote_copy(
            src_ref=src.at[rows_of(c)], dst_ref=from_mate.at[rows_of(c)],
            send_sem=so.at[c], recv_sem=ro.at[c], device_id={"tp": mate}, device_id_type=MESH)

    def copy_p(src, c):
        return pltpu.make_async_remote_copy(
            src_ref=src.at[rows_of(c)], dst_ref=from_peer.at[rows_of(c)],
            send_sem=sp.at[c], recv_sem=rp.at[c], device_id={"tp": peer}, device_id_type=MESH)

    def out_copy(src, c):
        return pltpu.make_async_copy(src.at[rows_of(c)], go_out.at[rows_of(c)], out_sem.at[c])

    def hop(src, dst, send, recv, t, to):
        return pltpu.make_async_remote_copy(
            src_ref=src.at[t], dst_ref=dst.at[t], send_sem=send.at[t], recv_sem=recv.at[t],
            device_id={"dp": to}, device_id_type=MESH)

    gq_copy.wait()
    half = tokens // 2
    for m in range(2):
        for t in range(TILES):
            if m == 0:
                w_copy(t).wait()
            c = slice(t * cols, (t + 1) * cols)
            r = slice(m * half, (m + 1) * half)
            part[r, c] = jnp.dot(gqv[r, :], wv[:, c], preferred_element_type=F32).astype(BF16)
        if m == 0:
            pl.semaphore_wait(barrier, n_dp - 1 + n_tp - 1)

        @pl.when(is_outer)
        def _():
            @pl.loop(m * steps // 2, (m + 1) * steps // 2)
            def _(k):
                copy_o(part, 2 * k + 1 - h).start()
                copy_o(part, 2 * k + h).start()

    gain_f = gain[...].astype(F32)
    r_copy.wait()

    @pl.loop(0, chunks)
    def _(c):
        r = rows_of(c)
        nv[r, :] = norm_rows(rv[r, :], gain_f)[2]

    gq_t[...] = gqv[...].T
    for v in range(2):
        for j, rel in enumerate(((0, 2, 1, 3), (0, 1, 2, 3))[v]):
            y_to = yy + (rel // 2) * (1 - 2 * yy)
            x_to = xx + (rel % 2) * (1 - 2 * xx)
            for mine in range(2):
                c_to = core if mine else 1 - core
                at = pl.multiple_of((y_to * 4 + x_to * 2 + c_to) * block, block)
                gq_p[v, mine, j * block:(j + 1) * block, :] = gq_t[pl.ds(at, block), :]
    gacc[...] = jnp.zeros_like(gacc)
    first, second = (x_mate, y_mate), (y_mate, x_mate)

    def tile_cols(t):
        return pl.ds(pl.multiple_of(t * cols, cols), cols)

    @pl.loop(0, TILES // 2)
    def _(j):
        for v in range(2):
            t = 2 * j + v
            fgs[t] = jnp.dot(gq_p[v, 0], nv[:, tile_cols(t)], preferred_element_type=F32).astype(BF16)
            hop(fgs, fgr, s1, r1, t, core_mate).start()

    def stage2(j):
        for v in range(2):
            t = 2 * j + v
            hop(fgs, fgr, s1, r1, t, core_mate).wait_recv()
            total = jnp.dot(gq_p[v, 1], nv[:, tile_cols(t)], preferred_element_type=F32)
            total = total + fgr[t].astype(F32)
            xs[t] = total[2 * block:].astype(BF16)
            hop(xs, xr, s2, r2, t, first[v]).start()
            keep[t] = total[:2 * block]

    def stage3(j):
        for v in range(2):
            t = 2 * j + v
            hop(xs, xr, s2, r2, t, first[v]).wait_recv()
            ys[t] = (keep[t, block:] + xr[t, block:].astype(F32)).astype(BF16)
            hop(ys, yr, s3, r3, t, second[v]).start()
            keep[t, :block] = keep[t, :block] + xr[t, :block].astype(F32)

    def wg_copy(t):
        return pltpu.make_async_copy(wgo.at[t], wg_out.at[:, tile_cols(t)], wg_sem.at[t])

    def stage4(j):
        for v in range(2):
            t = 2 * j + v
            hop(ys, yr, s3, r3, t, second[v]).wait_recv()
            wgo[t] = keep[t, :block] + yr[t].astype(F32)
            wg_copy(t).start()

    gi_copy.wait()

    def forward(k):
        b = 2 * k + 1 - h
        copy_p(from_peer, b).wait_recv()
        copy_o(from_peer, b).start()
        out_copy(from_peer, b).start()

    def collect(k):
        for c in (2 * k + h, 2 * k + 1 - h):
            copy_o(from_mate, c).wait_recv()
            out_copy(from_mate, c).start()

    def pass_on(k):
        b = rows_of(2 * k + 1 - h)
        copy_o(part, 2 * k + 1 - h).wait_recv()
        part[b, :] = (part[b, :].astype(F32) + from_mate[b, :].astype(F32)).astype(BF16)
        copy_p(part, 2 * k + 1 - h).start()

    def finish(k):
        a = 2 * k + h
        copy_o(part, a).wait_recv()
        copy_p(part, a).wait_recv()
        r = rows_of(a)
        inv_rms, unit, _ = norm_rows(rv[r, :], gain_f)
        dnormed = part[r, :].astype(F32) + from_mate[r, :].astype(F32)
        dnormed = dnormed + from_peer[r, :].astype(F32)
        gacc[...] += jnp.sum(dnormed * unit, axis=0, keepdims=True)
        dunit = dnormed * gain_f
        mean = jnp.mean(dunit * unit, axis=-1, keepdims=True)
        part[r, :] = (
            giv[r, :].astype(F32) + inv_rms * (dunit - unit * mean)
        ).astype(BF16)
        copy_p(part, a).start()
        copy_o(part, a).start()
        out_copy(part, a).start()

    @pl.loop(0, steps + 1)
    def _(k):
        @pl.when(jnp.logical_and(is_inner, k < steps))
        def _():
            pass_on(k)

        @pl.when(jnp.logical_and(is_inner, k > 0))
        def _():
            finish(k - 1)

        @pl.when(jnp.logical_and(is_inner, k > 1))
        def _():
            forward(k - 2)

        @pl.when(jnp.logical_and(is_outer, k > 2))
        def _():
            collect(k - 3)

        @pl.when(k < 2)
        def _():
            stage2(2 * k)
            stage2(2 * k + 1)

        @pl.when(jnp.logical_and(k >= 2, k < 2 + TILES // 2))
        def _():
            stage3(k - 2)

        @pl.when(jnp.logical_and(k >= 4, k < 4 + TILES // 2))
        def _():
            stage4(k - 4)

    def g_copy(o):
        return pltpu.make_async_remote_copy(
            src_ref=gslot.at[0], dst_ref=gslot.at[o], send_sem=sg.at[o], recv_sem=rg.at[o],
            device_id={"dp": (dp + o) % n_dp}, device_id_type=MESH)

    def z_copy(i, to):
        return pltpu.make_async_remote_copy(
            src_ref=gz.at[h], dst_ref=gz.at[h], send_sem=sz.at[i], recv_sem=rz.at[h],
            device_id={"tp": to}, device_id_type=MESH)

    def z_wait(which):
        pltpu.make_async_remote_copy(
            src_ref=gz.at[which], dst_ref=gz.at[which], send_sem=sz.at[0], recv_sem=rz.at[which],
            device_id={"tp": mate}, device_id_type=MESH).wait_recv()

    @pl.when(is_inner)
    def _():
        gslot[0] = gacc[...]
        for o in range(1, n_dp):
            g_copy(o).start()
        forward(steps - 1)
        for o in range(1, n_dp):
            g_copy(o).wait_recv()
        total = gslot[dp % n_dp]
        for d in range(1, n_dp):
            total = total + gslot[(dp + n_dp - d) % n_dp]
        gz[h] = total
        targets = (mate, peer, (1 - h) * (n_tp - 1))
        for i, to in enumerate(targets):
            z_copy(i, to).start()
        z_wait(1 - h)
        gg_out[...] = gz[0] + gz[1]
        for i, to in enumerate(targets):
            z_copy(i, to).wait_send()
        for o in range(1, n_dp):
            g_copy(o).wait_send()

        @pl.loop(0, chunks)
        def _(c):
            copy_p(part, c).wait_send()

    @pl.when(is_outer)
    def _():
        for k in range(steps - 2, steps):
            collect(k)
        z_wait(0)
        z_wait(1)
        gg_out[...] = gz[0] + gz[1]

    @pl.loop(0, chunks)
    def _(c):
        copy_o(part, c).wait_send()
        out_copy(part, c).wait()

    for t in range(TILES):
        hop(fgs, fgr, s1, r1, t, core_mate).wait_send()
        hop(xs, xr, s2, r2, t, first[t % 2]).wait_send()
        hop(ys, yr, s3, r3, t, second[t % 2]).wait_send()
        wg_copy(t).wait()


def fused(n_dp, n_tp, resid, gain, grad_q, w_query, grad_in):
    tokens, width = resid.shape
    heads = grad_q.shape[1]
    chunks = tokens // ROWS
    block, cols = heads // n_dp, width // TILES
    any_space = pl.BlockSpec(memory_space=pl.ANY)
    vmem = pl.BlockSpec(memory_space=pltpu.VMEM)
    dma = lambda n: pltpu.SemaphoreType.DMA((n,))
    weight_grad, gain_grad, grad_rows = pl.pallas_call(
        functools.partial(kernel, n_dp, n_tp),
        out_shape=(
            jax.ShapeDtypeStruct((block, width), F32),
            jax.ShapeDtypeStruct((1, width), F32),
            jax.ShapeDtypeStruct((tokens, width), BF16),
        ),
        in_specs=[any_space, vmem, any_space, any_space, any_space],
        out_specs=(any_space, vmem, any_space),
        scratch_shapes=[
            pltpu.VMEM((heads, width), BF16),
            pltpu.VMEM((tokens, width), BF16),
            pltpu.VMEM((tokens, heads), BF16),
            pltpu.VMEM((tokens, width), BF16),
            pltpu.VMEM((tokens, width), BF16),
            pltpu.VMEM((tokens, width), BF16),
            pltpu.VMEM((tokens, width), BF16),
            pltpu.VMEM((tokens, width), BF16),
            pltpu.VMEM((heads, tokens), BF16),
            pltpu.VMEM((2, 2, 4 * block, tokens), BF16),
            pltpu.VMEM((TILES, 4 * block, cols), BF16),
            pltpu.VMEM((TILES, 4 * block, cols), BF16),
            pltpu.VMEM((TILES, 2 * block, cols), F32),
            pltpu.VMEM((TILES, 2 * block, cols), BF16),
            pltpu.VMEM((TILES, 2 * block, cols), BF16),
            pltpu.VMEM((TILES, block, cols), BF16),
            pltpu.VMEM((TILES, block, cols), BF16),
            pltpu.VMEM((TILES, block, cols), F32),
            pltpu.VMEM((1, width), F32),
            pltpu.VMEM((n_dp, 1, width), F32),
            pltpu.VMEM((2, 1, width), F32),
            dma(TILES), dma(3), dma(chunks), dma(chunks), dma(chunks), dma(chunks), dma(chunks),
            dma(TILES), dma(TILES), dma(TILES), dma(TILES), dma(TILES), dma(TILES), dma(TILES),
            dma(n_dp), dma(n_dp), dma(3), dma(2),
        ],
        compiler_params=pltpu.CompilerParams(
            collective_id=0, has_side_effects=True, vmem_limit_bytes=60 * 1024 * 1024
        ),
    )(resid, gain.reshape(1, width), grad_q, w_query, grad_in)
    return weight_grad, gain_grad.reshape(width), grad_rows


def solution(mesh):
    n_dp, n_tp = mesh.shape["dp"], mesh.shape["tp"]
    if (n_dp, n_tp) == (2 * 2 * 2, 4):
        body = functools.partial(fused, n_dp, n_tp)
    else:
        body = per_device
    return jax.shard_map(
        body,
        mesh=mesh,
        in_specs=(P("dp", None), P(), P("dp", "tp"), P("tp", None), P("dp", None)),
        out_specs=(P(("tp", "dp"), None), P(), P("dp", None)),
        check_vma=False,
    )
```
